32 devices in a mesh: row: 4 (over z), col: 8 (over y, x, core).
Axes of the slice: x: 2, y: 2, z: 4, core: 2. Of those that a mesh axis runs over, the one named last changes fastest.
Arguments:
- tokens: bfloat16 [1024, 8192], P('row', 'col'), may hold values from -6 to 6
- gate_frozen_weight: bfloat16 [8192, 28672], P('col', 'row'), may hold values from -0.0625 to 0.0625
- gate_left_factor: bfloat16 [8192, 64], P('col'), may hold values from -0.046875 to 0.046875
- gate_right_factor: bfloat16 [64, 28672], P(None, 'row'), may hold values from -0.75 to 0.75
- gate_column_magnitude: float32 [28672], P('row'), may hold values from 0.5 to 1.5
- up_frozen_weight: bfloat16 [8192, 28672], P('col', 'row'), may hold values from -0.0625 to 0.0625
- up_left_factor: bfloat16 [8192, 64], P('col'), may hold values from -0.046875 to 0.046875
- up_right_factor: bfloat16 [64, 28672], P(None, 'row'), may hold values from -0.75 to 0.75
- up_column_magnitude: float32 [28672], P('row'), may hold values from 0.5 to 1.5
- down_frozen_weight: bfloat16 [28672, 8192], P('row', 'col'), may hold values from -0.03125 to 0.03125
- down_left_factor: bfloat16 [28672, 64], P('row'), may hold values from -0.02734375 to 0.02734375
- down_right_factor: bfloat16 [64, 8192], P(None, 'col'), may hold values from -0.75 to 0.75
- down_column_magnitude: float32 [8192], P('col'), may hold values from 0.5 to 1.5
Outputs:
- mixed: bfloat16 [1024, 8192], P('row', 'col')
The draws below stay inside these ranges and needn't reach their ends.
All inputs are finite; a program needn't handle non-finite values.
Results may differ from the reference program's by a relative error of at most 0.028.
Values may be sent and summed in bfloat16 or wider, within the bound.
No kernel may reach another device: no remote copies, remote signals or barrier semaphores. Data moves between devices by JAX's collectives and lax.ppermute only.
A program may use at most 192 MiB of HBM per device.

```python
import jax
import jax.numpy as jnp
from jax import lax

MODEL_WIDTH = 8192
HIDDEN_UNITS = 28672
UPDATE_RANK = 64
TOKENS = 1024
N_ROW = 4
N_COL = 8


def block_levels(own_key, shape, cuts, least, largest):
    def one(axis_at, parts):
        draws = jax.random.uniform(jax.random.fold_in(jax.random.fold_in(own_key, 6), axis_at), (parts,), jnp.float32, least / len(cuts), largest / len(cuts))
        return jnp.repeat(jnp.exp(draws), shape[axis_at] // parts).reshape((-1,) + (1,) * (len(shape) - axis_at - 1))

    loudness = one(*cuts[0])
    for cut in cuts[1:]:
        loudness = loudness * one(*cut)
    return loudness


def normal_values(own_key, shape, deviation, bound, cuts=(), kind=jnp.bfloat16):
    result = deviation * jax.random.normal(own_key, shape, jnp.float32)
    if cuts:
        result = result * block_levels(own_key, shape, cuts, -0.22, 0.18)
    return jnp.clip(result, -bound, bound).astype(kind)


def setup_inputs(seed: int = 0) -> dict:
    keys = jax.random.split(jax.random.key(seed), 14)
    tokens = normal_values(keys[0], (TOKENS, MODEL_WIDTH), 1.0, 6.0, ((0, 4), (1, 8)))
    gate_frozen_weight = normal_values(keys[1], (MODEL_WIDTH, HIDDEN_UNITS), MODEL_WIDTH ** -0.5, 0.0625, ((0, 8), (1, 4)))
    gate_left_factor = normal_values(keys[2], (MODEL_WIDTH, UPDATE_RANK), (0.3 * MODEL_WIDTH ** -0.5), 0.046875, ((0, 8),))
    gate_right_factor = normal_values(keys[3], (UPDATE_RANK, HIDDEN_UNITS), UPDATE_RANK ** -0.5, 0.75, ((1, 4),))
    gate_column_magnitude = jnp.clip(1.0 + 0.1 * jax.random.normal(keys[4], (HIDDEN_UNITS,), jnp.float32), 0.5, 1.5)
    up_frozen_weight = normal_values(keys[5], (MODEL_WIDTH, HIDDEN_UNITS), MODEL_WIDTH ** -0.5, 0.0625, ((0, 8), (1, 4)))
    up_left_factor = normal_values(keys[6], (MODEL_WIDTH, UPDATE_RANK), (0.3 * MODEL_WIDTH ** -0.5), 0.046875, ((0, 8),))
    up_right_factor = normal_values(keys[7], (UPDATE_RANK, HIDDEN_UNITS), UPDATE_RANK ** -0.5, 0.75, ((1, 4),))
    up_column_magnitude = jnp.clip(1.0 + 0.1 * jax.random.normal(keys[8], (HIDDEN_UNITS,), jnp.float32), 0.5, 1.5)
    down_frozen_weight = normal_values(keys[9], (HIDDEN_UNITS, MODEL_WIDTH), HIDDEN_UNITS ** -0.5, 0.03125, ((0, 4), (1, 8)))
    down_left_factor = normal_values(keys[10], (HIDDEN_UNITS, UPDATE_RANK), (0.3 * HIDDEN_UNITS ** -0.5), 0.02734375, ((0, 4),))
    down_right_factor = normal_values(keys[11], (UPDATE_RANK, MODEL_WIDTH), UPDATE_RANK ** -0.5, 0.75, ((1, 8),))
    down_column_magnitude = jnp.clip(1.0 + 0.1 * jax.random.normal(keys[12], (MODEL_WIDTH,), jnp.float32), 0.5, 1.5)
    return dict(tokens=tokens, gate_frozen_weight=gate_frozen_weight, gate_left_factor=gate_left_factor, gate_right_factor=gate_right_factor, gate_column_magnitude=gate_column_magnitude, up_frozen_weight=up_frozen_weight, up_left_factor=up_left_factor, up_right_factor=up_right_factor, up_column_magnitude=up_column_magnitude, down_frozen_weight=down_frozen_weight, down_left_factor=down_left_factor, down_right_factor=down_right_factor, down_column_magnitude=down_column_magnitude)


stability_offset = 1e-06

def column_square_totals(weight, low_b, low_a, blocks):
    height, width = weight.shape
    piece = width // blocks
    weight_blocks = weight.reshape(height, blocks, piece).transpose(1, 0, 2)
    factor_blocks = low_a.reshape(low_a.shape[0], blocks, piece).transpose(1, 0, 2)

    def single(pair):
        merged = pair[0].astype(jnp.float32) + jnp.dot(low_b, pair[1], preferred_element_type=jnp.float32)
        return lax.optimization_barrier(jnp.sum(merged * merged, axis=0))
    return lax.map(single, (weight_blocks, factor_blocks)).reshape(width)

def blocked_direct(inputs, weight, blocks):
    piece = inputs.shape[1] // blocks

    def step(index, total):
        start = (index * piece).astype(jnp.int32)
        left = lax.dynamic_slice_in_dim(inputs, start, piece, 1)
        right = lax.dynamic_slice_in_dim(weight, start, piece, 0)
        rounded = jnp.dot(left, right, preferred_element_type=jnp.float32).astype(jnp.bfloat16)
        rounded = lax.optimization_barrier(rounded)
        return total + rounded.astype(jnp.float32)
    start_total = jnp.zeros((inputs.shape[0], weight.shape[1]), jnp.float32)
    return lax.fori_loop(0, blocks, step, start_total)

def adapted_input(inputs, weight, low_b, low_a, scale):
    direct = blocked_direct(inputs, weight, N_COL)
    coords = jnp.dot(inputs, low_b, preferred_element_type=jnp.float32)
    update = jnp.dot(coords, low_a.astype(jnp.float32), precision=lax.Precision.HIGHEST)
    return (direct + update) * scale[None, :]

def adapted_matrix(inputs, weight, low_b, low_a, scale):
    direct = jnp.dot(inputs, weight, preferred_element_type=jnp.float32)
    coords = jnp.dot(inputs, low_b, preferred_element_type=jnp.float32)
    update = jnp.dot(coords, low_a.astype(jnp.float32), precision=lax.Precision.HIGHEST)
    return (direct + update) * scale[None, :]

def reference(tokens, gate_frozen_weight, gate_left_factor, gate_right_factor, gate_column_magnitude, up_frozen_weight, up_left_factor, up_right_factor, up_column_magnitude, down_frozen_weight, down_left_factor, down_right_factor, down_column_magnitude):
    gate_column_scale = gate_column_magnitude / jnp.sqrt(column_square_totals(gate_frozen_weight, gate_left_factor, gate_right_factor, N_ROW) + stability_offset)
    up_column_scale = up_column_magnitude / jnp.sqrt(column_square_totals(up_frozen_weight, up_left_factor, up_right_factor, N_ROW) + stability_offset)
    down_column_scale = down_column_magnitude / jnp.sqrt(column_square_totals(down_frozen_weight, down_left_factor, down_right_factor, N_COL) + stability_offset)
    gate_preactivation = adapted_input(tokens, gate_frozen_weight, gate_left_factor, gate_right_factor, gate_column_scale)
    up_preactivation = adapted_input(tokens, up_frozen_weight, up_left_factor, up_right_factor, up_column_scale)
    hidden_values = (jax.nn.silu(gate_preactivation) * up_preactivation).astype(jnp.bfloat16)
    mixed = adapted_matrix(hidden_values, down_frozen_weight, down_left_factor, down_right_factor, down_column_scale)
    return mixed.astype(jnp.bfloat16)
```

```python
import jax
import jax.numpy as jnp
from jax import lax
from jax.experimental import pallas as pl
from jax.experimental.pallas import tpu as pltpu
from jax.sharding import PartitionSpec as P

stability_offset = 1e-06


def block_of(size, choices):
    for choice in choices:
        if size % choice == 0:
            return choice
    return size


def merge_body(weight, left, right, merged_out, square_out):
    merged = weight[...].astype(jnp.float32) + jnp.dot(
        left[...], right[...], preferred_element_type=jnp.float32
    )
    merged_out[...] = merged.astype(jnp.bfloat16)

    @pl.when(pl.program_id(1) == 0)
    def _():
        square_out[...] = jnp.zeros_like(square_out)

    square_out[...] += jnp.sum(merged * merged, axis=0, keepdims=True)


def merge(weight, left, right):
    height, width = weight.shape
    rank = left.shape[1]
    tall = block_of(height, (1024, 512, 256, 128))
    wide = block_of(width, (512, 256, 128))
    merged, squares = pl.pallas_call(
        merge_body,
        grid=(width // wide, height // tall),
        in_specs=[
            pl.BlockSpec((tall, wide), lambda j, i: (i, j)),
            pl.BlockSpec((tall, rank), lambda j, i: (i, 0)),
            pl.BlockSpec((rank, wide), lambda j, i: (0, j)),
        ],
        out_specs=[
            pl.BlockSpec((tall, wide), lambda j, i: (i, j)),
            pl.BlockSpec((1, wide), lambda j, i: (0, j)),
        ],
        out_shape=[
            jax.ShapeDtypeStruct((height, width), jnp.bfloat16),
            jax.ShapeDtypeStruct((1, width), jnp.float32),
        ],
        compiler_params=pltpu.CompilerParams(dimension_semantics=("arbitrary", "arbitrary")),
    )(weight, left, right)
    return merged, squares[0]


def flip(value, axis, bit):
    count = lax.axis_size(axis)
    return lax.ppermute(value, axis, [(i, i ^ (1 << bit)) for i in range(count)])


def total_over(value, axis):
    for bit in range(lax.axis_size(axis).bit_length() - 1):
        value = value + flip(value, axis, bit)
    return value


def my_bit(axis, bit):
    return (lax.axis_index(axis) >> bit) & 1


def scatter_sum(part, axis, order):
    left = sorted(order, reverse=True)
    terms = [part]
    for bit in order:
        at = left.index(bit)
        mine = my_bit(axis, bit)

        def pick(term, which):
            return lax.dynamic_index_in_dim(term, which, at, keepdims=False)

        send = sum(pick(term, 1 - mine).astype(jnp.float32) for term in terms)
        received = flip(send.astype(jnp.bfloat16), axis, bit)
        terms = [pick(term, mine) for term in terms] + [received]
        left.remove(bit)
    return sum(term.astype(jnp.float32) for term in terms)


def gather_all(value, axis, order):
    for bit in order:
        received = flip(value, axis, bit)
        mine = my_bit(axis, bit) == 0
        value = jnp.stack(
            [jnp.where(mine, value, received), jnp.where(mine, received, value)], axis=0
        )
    return value


def shards(
    tokens,
    gate_frozen_weight,
    gate_left_factor,
    gate_right_factor,
    gate_column_magnitude,
    up_frozen_weight,
    up_left_factor,
    up_right_factor,
    up_column_magnitude,
    down_frozen_weight,
    down_left_factor,
    down_right_factor,
    down_column_magnitude,
):
    rows = lax.axis_size("row")
    cols = lax.axis_size("col")
    bits = cols.bit_length() - 1
    halves = (2,) * bits
    count = tokens.shape[0]
    own = count // cols
    rising = tuple(range(1, bits))
    falling = rising[::-1]

    blocks = [tokens] + [
        lax.ppermute(tokens, "row", [((i + s) % rows, i) for i in range(rows)])
        for s in range(1, rows)
    ]
    gate_weight, gate_sq = merge(gate_frozen_weight, gate_left_factor, gate_right_factor)
    up_weight, up_sq = merge(up_frozen_weight, up_left_factor, up_right_factor)
    down_weight, down_sq = merge(down_frozen_weight, down_left_factor, down_right_factor)
    both_sq = total_over(jnp.stack([gate_sq, up_sq]), "col")
    gate_scale = gate_column_magnitude / jnp.sqrt(both_sq[0] + stability_offset)
    up_scale = up_column_magnitude / jnp.sqrt(both_sq[1] + stability_offset)
    down_scale = down_column_magnitude / jnp.sqrt(
        total_over(down_sq, "row") + stability_offset
    )

    def partial_of(block, weight):
        part = jnp.dot(block, weight, preferred_element_type=jnp.float32).astype(jnp.bfloat16)
        return part.reshape(halves + (own, weight.shape[1]))

    mixed = None
    for s, block in enumerate(blocks):
        gate = scatter_sum(partial_of(block, gate_weight), "col", (0,) + rising)
        up = scatter_sum(partial_of(block, up_weight), "col", (0,) + falling)
        hidden = (
            jax.nn.silu(gate * gate_scale[None, :]) * (up * up_scale[None, :])
        ).astype(jnp.bfloat16)
        order = (rising if s % 2 == 0 else falling) + (0,)
        full = gather_all(hidden, "col", order).reshape(count, hidden.shape[1])
        down = jnp.dot(full, down_weight, preferred_element_type=jnp.float32)
        down = down.astype(jnp.bfloat16).reshape(halves + (own, down_weight.shape[1]))
        held = order[::-1]
        down = jnp.transpose(
            down, tuple(held.index(b) for b in range(bits - 1, -1, -1)) + (bits, bits + 1)
        ).reshape(count, down_weight.shape[1])
        if s:
            down = lax.ppermute(down, "row", [(i, (i + s) % rows) for i in range(rows)])
        down = down.astype(jnp.float32)
        mixed = down if mixed is None else mixed + down
    return (mixed * down_scale[None, :]).astype(jnp.bfloat16)


def solution(mesh):
    placed = (
        P("row", "col"),
        P("col", "row"),
        P("col", None),
        P(None, "row"),
        P("row"),
        P("col", "row"),
        P("col", None),
        P(None, "row"),
        P("row"),
        P("row", "col"),
        P("row", None),
        P(None, "col"),
        P("col"),
    )
    return jax.shard_map(
        shards, mesh=mesh, in_specs=placed, out_specs=P("row", "col"), check_vma=False
    )
```
